32 devices in a mesh: node: 32 (over z, y, x, core).
Axes of the slice: x: 2, y: 2, z: 4, core: 2. Of those that a mesh axis runs over, the one named last changes fastest.
Arguments:
- round_index: int32 [1], replicated, may hold values from 0 to 63
- sample_ids: int32 [32, 8], P('node'), may hold values from 0 to 3
- token_pool: bfloat16 [32, 4, 64, 512], P('node'), may hold values from -20 to 20
- cotangent_pool: bfloat16 [32, 4, 64, 512], P('node'), may hold values from -6 to 6
- weights: bfloat16 [32, 4, 512, 512], P('node'), may hold values from -12 to 12
- residue: bfloat16 [32, 4, 512, 512], P('node'), may hold values from -6 to 6
Outputs:
- new_weights: bfloat16 [32, 4, 512, 512], P('node')
- new_residue: bfloat16 [32, 4, 512, 512], P('node')
- grad_rms: float32 [], replicated
The draws below stay inside these ranges and needn't reach their ends.
All inputs are finite; a program needn't handle non-finite values.
Results may differ from the reference program's by a relative error of at most 0.0065.
Values may be sent and summed in bfloat16 or wider, within the bound.
A program may use at most 128 MiB of HBM per device.

```python
import jax
import jax.numpy as jnp
from jax import lax

HEAD_DIM = 64
D = 512
SEQ = 64
BATCH = 8
POOL = 4
NODES = 32
N_NODE = 32


def draw_weights(key, part):
    shape_all = (NODES, 4, D, D)
    drawn = jax.random.normal(key, shape_all, jnp.float32)
    return jnp.clip(drawn, -12.0, 12.0).astype(jnp.bfloat16)


def draw_token_pool(key, part):
    shape_all = (NODES, POOL, SEQ, D)
    drawn = jax.random.normal(key, shape_all, jnp.float32)
    return jnp.clip(drawn, -20.0, 20.0).astype(jnp.bfloat16)


def draw_cotangent_pool(key, part):
    shape_all = (NODES, POOL, SEQ, D)
    rising = (jnp.arange(NODES, dtype=jnp.float32) / max(NODES - 1, 1)).reshape(NODES, 1, 1, 1)
    drawn = jax.random.normal(key, shape_all, jnp.float32) * 0.5 * jnp.power(3.0, 0.5 * rising)
    return jnp.clip(drawn, -6.0, 6.0).astype(jnp.bfloat16)


def place_ends(values, stream_key, smallest, high):
    longest = values.shape.index(max(values.shape))
    spots = []
    for shift in (0, 1):
        where = [jax.random.randint(jax.random.fold_in(stream_key, axis), (), 0, length) for axis, length in enumerate(values.shape)]
        where[longest] = (where[longest] + shift) % values.shape[longest]
        spots.append(tuple(where))
    return values.at[spots[0]].set(smallest).at[spots[1]].set(high)


def steps_of(stream_key, extent, cuts, smallest, top_value):
    gain, own = 1.0, jax.random.fold_in(stream_key, 6)
    for axis_at, parts in cuts:
        heights = jnp.exp(jax.random.uniform(jax.random.fold_in(own, axis_at), (parts,), jnp.float32, smallest / len(cuts), top_value / len(cuts)))
        gain = gain * jnp.repeat(heights, extent[axis_at] // parts).reshape([-1 if axis == axis_at else 1 for axis in range(len(extent))])
    return gain


def centred(own_key, dims, scale, most, shards=(), held_as=jnp.bfloat16):
    entries = jax.random.normal(own_key, dims, jnp.float32) * scale
    if len(shards) > 0:
        entries = steps_of(own_key, dims, shards, -0.22, 0.18) * entries
    return jnp.clip(entries, min=-most, max=most).astype(held_as)


def setup_inputs(seed: int = 0) -> dict:
    keys = jax.random.split(jax.random.key(seed), 7)
    round_index = jax.random.randint(keys[0], (1,), 0, 64).astype(jnp.int32)
    sample_ids = place_ends(jax.random.randint(keys[1], (NODES, BATCH), 0, POOL), jax.random.fold_in(keys[1], 1), 0, POOL - 1).astype(jnp.int32)
    token_pool = draw_token_pool(jax.random.fold_in(keys[6], 71), 0)
    cotangent_pool = draw_cotangent_pool(jax.random.fold_in(keys[6], 71), 0)
    weights = draw_weights(jax.random.fold_in(keys[6], 71), 0)
    residue = centred(keys[5], (NODES, 4, D, D), 1.0, 6.0, ((0, 32),))
    return {"round_index": round_index, "sample_ids": sample_ids, "token_pool": token_pool, "cotangent_pool": cotangent_pool, "weights": weights, "residue": residue}


epsilon = 1e-06
step_rate = 0.1

def normalize(tokens):
    values = tokens.astype(jnp.float32)
    centered = values - lax.optimization_barrier(jnp.mean(values, -1, keepdims=True))
    variance = lax.optimization_barrier(jnp.mean(centered * centered, -1, keepdims=True))
    return (centered * lax.rsqrt(variance + epsilon)).astype(jnp.bfloat16)

def node_gradient(weights, tokens, cotangent):
    batch_size, seq_len, model_width = tokens.shape
    head_count = model_width // HEAD_DIM
    proj_scale = model_width ** (-0.5)
    head_scale = HEAD_DIM ** (-0.5)
    row_count = batch_size * seq_len
    normed_rows = normalize(tokens).reshape(row_count, model_width)
    grad_rows = cotangent.reshape(row_count, model_width)

    def project(which):
        return (jnp.dot(normed_rows, weights[which], preferred_element_type=jnp.float32) * proj_scale).astype(jnp.bfloat16)

    def to_heads(matrix):
        return matrix.reshape(batch_size, seq_len, head_count, HEAD_DIM).astype(jnp.float32)
    queries = to_heads(project(0))
    key_rows = to_heads(project(1))
    value_rows = to_heads(project(2))
    scores = jnp.einsum('bshe,bthe->bhst', queries, key_rows) * head_scale
    attn_probs = jnp.exp(scores - lax.optimization_barrier(jnp.max(scores, -1, keepdims=True)))
    attn_probs = attn_probs / lax.optimization_barrier(jnp.sum(attn_probs, -1, keepdims=True))
    probs_half = attn_probs.astype(jnp.bfloat16).astype(jnp.float32)
    context = jnp.einsum('bhst,bthe->bshe', probs_half, value_rows).astype(jnp.bfloat16).reshape(row_count, model_width)
    grad_out = jnp.dot(context.T, grad_rows, preferred_element_type=jnp.float32) * proj_scale
    context_grad = (jnp.dot(grad_rows, weights[3].T, preferred_element_type=jnp.float32) * proj_scale).astype(jnp.bfloat16)
    context_heads = to_heads(context_grad)
    probs_grad = jnp.einsum('bshe,bthe->bhst', context_heads, value_rows)
    value_grad = jnp.einsum('bhst,bshe->bthe', probs_half, context_heads).astype(jnp.bfloat16)
    score_grad = (attn_probs * (probs_grad - lax.optimization_barrier(jnp.sum(probs_grad * attn_probs, -1, keepdims=True))) * head_scale).astype(jnp.bfloat16).astype(jnp.float32)
    query_grad = jnp.einsum('bhst,bthe->bshe', score_grad, key_rows).astype(jnp.bfloat16)
    key_grad = jnp.einsum('bhst,bshe->bthe', score_grad, queries).astype(jnp.bfloat16)

    def weight_grad(rows_grad):
        return jnp.dot(normed_rows.T, rows_grad.reshape(row_count, model_width), preferred_element_type=jnp.float32) * proj_scale
    return jnp.stack([weight_grad(query_grad), weight_grad(key_grad), weight_grad(value_grad), grad_out])

def reference(round_index, sample_ids, token_pool, cotangent_pool, weights, residue):

    def per_node(node_index):
        sample_rows = sample_ids[node_index]
        tokens = jnp.take(token_pool[node_index], sample_rows, axis=0)
        cotangent = jnp.take(cotangent_pool[node_index], sample_rows, axis=0)
        gradient = node_gradient(weights[node_index], tokens, cotangent)
        tracked = (residue[node_index].astype(jnp.float32) + gradient).astype(jnp.bfloat16)
        return (tracked, gradient, jnp.sum(gradient * gradient))
    tracked, gradient, squares = lax.map(per_node, jnp.arange(N_NODE, dtype=jnp.int32))
    levels = N_NODE.bit_length() - 1
    offset = jnp.left_shift(jnp.int32(1), round_index[0] % levels)

    def track_node(node_index):
        peer_index = (node_index - offset) % N_NODE
        tracker = 0.5 * (tracked[node_index].astype(jnp.float32) + tracked[peer_index].astype(jnp.float32))
        sent = (weights[node_index].astype(jnp.float32) - step_rate * tracker).astype(jnp.bfloat16)
        return (tracker, sent)
    tracker_all, sent_all = lax.map(track_node, jnp.arange(N_NODE, dtype=jnp.int32))

    def mix_node(node_index):
        peer_index = (node_index - offset) % N_NODE
        tracker = tracker_all[node_index]
        mixed = 0.5 * weights[node_index].astype(jnp.float32) + 0.5 * sent_all[peer_index].astype(jnp.float32) - 0.5 * step_rate * tracker
        return (mixed.astype(jnp.bfloat16), (tracker - gradient[node_index]).astype(jnp.bfloat16))
    new_weights, new_residue = lax.map(mix_node, jnp.arange(N_NODE, dtype=jnp.int32))
    grad_rms = jnp.sqrt(jnp.sum(squares) / (N_NODE * gradient[0].size))
    return (new_weights, new_residue, grad_rms)
```

```python
from functools import partial

import jax
import jax.numpy as jnp
from jax import lax
from jax.experimental import pallas as pl
from jax.experimental.pallas import tpu as pltpu
from jax.sharding import PartitionSpec as P

HEAD_DIM = 64
LANES = 128
CHUNK_ROWS = 128

epsilon = 1e-06
step_rate = 0.1

f32, bf16 = jnp.float32, jnp.bfloat16
MESH = pl.DeviceIdType.MESH
VMEM = pl.BlockSpec(memory_space=pltpu.VMEM)
HBM = pl.BlockSpec(memory_space=pltpu.HBM)


def dot(left, right, left_dim=1, right_dim=0):
    return lax.dot_general(
        left, right, (((left_dim,), (right_dim,)), ((), ())), preferred_element_type=f32
    )


def round_kernel(
    nodes,
    offset,
    ids_hbm,
    tokens_hbm,
    cot_hbm,
    weights_hbm,
    residue_hbm,
    new_weights_ref,
    new_residue_ref,
    rms_ref,
    ids_ref,
    tokens_ref,
    cot_ref,
    weights_ref,
    residue_ref,
    left_ref,
    right_ref,
    context_ref,
    gradient,
    tracked,
    tracked_in,
    sent,
    sent_in,
    squares,
    totals,
    totals_in,
    load_sems,
    track_send,
    track_recv,
    sent_send,
    sent_recv,
    sum_send,
    sum_recv,
):
    me = lax.axis_index("node")
    target = lax.rem(me + offset, nodes)
    source = lax.rem(me + nodes - offset, nodes)
    steps = nodes.bit_length() - 1
    mutual = 2 * offset == nodes
    strides = [2**k for k in range(steps)]
    if not mutual:
        strides = [offset] + [stride for stride in strides if stride != offset]
    partners = [me + stride * (1 - 2 * ((me // stride) % 2)) for stride in strides]

    barrier = pltpu.get_barrier_semaphore()
    for other in [target, source] + partners:
        pl.semaphore_signal(barrier, inc=1, device_id=(other,), device_id_type=MESH)

    pool, seq, width = tokens_ref.shape
    matrices = weights_ref.shape[0]
    rows = pool * seq
    pairs = width // LANES
    per_matrix = width // CHUNK_ROWS
    proj_scale = width**-0.5
    head_scale = HEAD_DIM**-0.5
    order = [3, 2, 0, 1]

    moves = {"tokens": (tokens_hbm.at[0], tokens_ref), "cot": (cot_hbm.at[0], cot_ref)}
    moves["ids"] = (ids_hbm, ids_ref)
    head_cols, rest_cols = pl.ds(0, LANES), pl.ds(LANES, width - LANES)
    head_rows, rest_rows = pl.ds(0, CHUNK_ROWS), pl.ds(CHUNK_ROWS, width - CHUNK_ROWS)
    for m in range(3):
        moves["w", m] = (weights_hbm.at[0, m, :, head_cols], weights_ref.at[m, :, head_cols])
        moves["w+", m] = (weights_hbm.at[0, m, :, rest_cols], weights_ref.at[m, :, rest_cols])
        moves["r", m] = (residue_hbm.at[0, m], residue_ref.at[m])
    moves["w", 3] = (weights_hbm.at[0, 3], weights_ref.at[3])
    moves["r", 3] = (residue_hbm.at[0, 3, head_rows], residue_ref.at[3, head_rows])
    moves["r+", 3] = (residue_hbm.at[0, 3, rest_rows], residue_ref.at[3, rest_rows])
    when = ["tokens", ("w", 0), ("w", 1), ("w", 2), "ids", "cot", ("r", 3), ("w+", 0), ("w+", 1), ("w+", 2), ("r+", 3)]
    when += [("w", 3), ("r", 2), ("r", 0), ("r", 1)]
    loads = {name: pltpu.make_async_copy(*moves[name], load_sems.at[n]) for n, name in enumerate(when)}
    for name in when:
        loads[name].start()

    def track_copy(c):
        return pltpu.make_async_remote_copy(
            tracked.at[c], tracked_in.at[c], track_send.at[c], track_recv.at[c], (target,), MESH
        )

    def sent_copy(c):
        return pltpu.make_async_remote_copy(
            sent.at[c], sent_in.at[c], sent_send.at[c], sent_recv.at[c], (target,), MESH
        )

    def weights_copy(m, part, c):
        return pltpu.make_async_remote_copy(
            weights_hbm.at[0, m, part],
            sent_in.at[c],
            sent_send.at[c],
            sent_recv.at[c],
            (target,),
            MESH,
        )

    def each_block(which, body):
        for m in which:

            @pl.loop(0, per_matrix)
            def _(r):
                body(m, pl.ds(r * CHUNK_ROWS, CHUNK_ROWS), order.index(m) * per_matrix + r)

    def send_weights(m, part, c):
        weights_copy(m, part, c).start()

    if mutual:
        pl.semaphore_wait(barrier, 2 + steps)
        each_block(order[:2], send_weights)

    loads["tokens"].wait()
    values = tokens_ref[...].reshape(rows, width).astype(f32)
    centered = values - jnp.mean(values, -1, keepdims=True)
    variance = jnp.mean(centered * centered, -1, keepdims=True)
    unit_rows = centered * lax.rsqrt(variance + epsilon)
    normed = unit_rows.astype(bf16)
    first = lax.broadcasted_iota(jnp.int32, (seq, LANES), 1) < HEAD_DIM
    units = [(i, j) for i in range(pool) for j in range(pairs)]
    spots = [
        (slice(i * seq, (i + 1) * seq), slice(j * LANES, (j + 1) * LANES)) for i, j in units
    ]

    def spread(block):
        zero = jnp.zeros_like(block)
        return jnp.concatenate([jnp.where(first, block, zero), jnp.where(first, zero, block)], 0)

    def gather(block):
        return jnp.where(first, block[:seq], block[seq:])

    def track(m, part, c):
        right = right_ref[m] if m < 3 else cot
        grad = dot(left_ref[m // 3, part], right) * proj_scale
        gradient[c] = grad
        tracked[c] = (residue_ref[m, part].astype(f32) + grad).astype(bf16)
        if mutual or m in order[:2]:
            track_copy(c).start()
        squares[...] += jnp.sum((grad * grad).reshape(-1, 8, width), 0)

    loads["ids"].wait()
    ids = ids_ref[...]
    counts = [jnp.sum((ids == image).astype(f32), 1, keepdims=True) for image in range(pool)]
    loads["cot"].wait()
    cot = cot_ref[...].reshape(rows, width)
    squares[...] = jnp.zeros_like(squares)
    queries2, keys1, vals1, probs, half = {}, {}, {}, {}, {}
    for j in range(pairs):
        cols = slice(j * LANES, (j + 1) * LANES)
        if j < 2:
            for m in range(3):
                loads["w+" if j else "w", m].wait()
        queries, keys, vals = [
            (dot(normed, weights_ref[m, :, cols]) * proj_scale).astype(bf16) for m in range(3)
        ]
        here = [(i, j) for i in range(pool)]
        for i, u in enumerate(here):
            part = slice(i * seq, (i + 1) * seq)
            queries2[u], keys1[u], vals1[u] = spread(queries[part]), keys[part], vals[part]
        scores = [dot(queries2[u], keys1[u], 1, 1) * head_scale for u in here]
        for u, score in zip(here, scores):
            e = jnp.exp(score - jnp.max(score, -1, keepdims=True))
            probs[u] = e / jnp.sum(e, -1, keepdims=True)
            half[u] = probs[u].astype(bf16)
        context = [gather(dot(half[u], vals1[u])) * counts[u[0]] for u in here]
        left_ref[1, cols] = jnp.concatenate(context, 0).T.astype(bf16)
        if j == 0 and not mutual:
            pl.semaphore_wait(barrier, 2 + steps)
        if j < 2:
            loads["r+" if j else "r", 3].wait()
        track(3, pl.ds(j * LANES, LANES), order.index(3) * per_matrix + j)

    loads["w", 3].wait()
    context_grad = (dot(cot, weights_ref[3], 1, 1) * proj_scale).astype(bf16)
    weighted = [unit_rows[i * seq : (i + 1) * seq] * counts[i] for i in range(pool)]
    left_ref[0] = jnp.concatenate(weighted, 0).T.astype(bf16)
    queries2, keys1, vals1, probs, half = [
        [found[u] for u in units] for found in (queries2, keys1, vals1, probs, half)
    ]
    grads2 = [spread(context_grad[at]) for at in spots]
    for n, at in enumerate(spots):
        right_ref[2, at[0], at[1]] = dot(half[n], grads2[n], 0, 0).astype(bf16)
    loads["r", 2].wait()
    each_block([2], track)
    probs_grad = [dot(g, v, 1, 1) for g, v in zip(grads2, vals1)]
    score_grad = []
    for p, g in zip(probs, probs_grad):
        inner = jnp.sum(g * p, -1, keepdims=True)
        score_grad.append((p * (g - inner) * head_scale).astype(bf16))
    for n, at in enumerate(spots):
        right_ref[0, at[0], at[1]] = gather(dot(score_grad[n], keys1[n])).astype(bf16)
        right_ref[1, at[0], at[1]] = dot(score_grad[n], queries2[n], 0, 0).astype(bf16)
    for m in order[2:]:
        loads["r", m].wait()
    each_block(order[2:], track)

    def sum_copy(k):
        return pltpu.make_async_remote_copy(
            totals.at[k], totals_in.at[k], sum_send.at[k], sum_recv.at[k], (partners[k],), MESH
        )

    def sum_finish(k):
        sum_copy(k).wait()
        totals[k + 1] = totals[k] + totals_in[k]

    own_total = jnp.sum(jnp.sum(squares[...], 0, keepdims=True), 1, keepdims=True)
    totals[0] = jnp.broadcast_to(own_total, totals.shape[1:])
    entries = nodes * matrices * width * width

    def set_rms():
        rms_ref[0] = jnp.sqrt(totals[steps] / entries)

    def mix(m, part, c):
        track_copy(c).wait_recv()
        tracker = 0.5 * (tracked[c].astype(f32) + tracked_in[c].astype(f32))
        own = weights_ref[m, part].astype(f32)
        new_residue_ref[0, m, part] = (tracker - gradient[c]).astype(bf16)
        base = 0.5 * own - 0.5 * step_rate * tracker
        if mutual:
            weights_copy(m, part, c).wait_recv()
            peer_sent = (sent_in[c].astype(f32) - step_rate * tracker).astype(bf16)
            new_weights_ref[0, m, part] = (base + 0.5 * peer_sent.astype(f32)).astype(bf16)
        else:
            sent[c] = (own - step_rate * tracker).astype(bf16)
            sent_copy(c).start()
            gradient[c] = base

    def finish(m, part, c):
        sent_copy(c).wait_recv()
        new_weights_ref[0, m, part] = (gradient[c] + 0.5 * sent_in[c].astype(f32)).astype(bf16)

    def drain(m, part, c):
        track_copy(c).wait_send()
        weights_copy(m, part, c).wait_send()

    def drain_sent(m, part, c):
        sent_copy(c).wait_send()

    if mutual:
        for k in range(steps - 2):
            sum_copy(k).start()
            sum_finish(k)
        for n, k in enumerate([steps - 2, steps - 1]):
            sum_copy(k).start()
            each_block([order[2 + n]], send_weights)
            each_block([order[n]], mix)
            sum_finish(k)
        set_rms()
        each_block(order[2:], mix)
        each_block(order, drain)
    else:
        chunks = matrices * per_matrix
        held = 2 * per_matrix
        lag = min(3, held)
        starts = [held + k * (chunks - held) // steps for k in range(steps)]
        for c in range(held, chunks):
            track_copy(c - lag).wait_send()
            for k in range(steps):
                if starts[k] == c:
                    if k:
                        sum_finish(k - 1)
                    sum_copy(k).start()
            track_copy(c).start()
        sum_finish(steps - 1)
        set_rms()
        each_block(order, mix)
        each_block(order, finish)
        for c in range(chunks):
            if c < held - lag or c >= chunks - lag:
                track_copy(c).wait_send()
        each_block(order, drain_sent)


def one_round(nodes, level, sample_ids, token_pool, cotangent_pool, weights, residue):
    pool, seq, width = token_pool.shape[1:]
    matrices = weights.shape[1]
    rows = pool * seq
    chunks = matrices * (width // CHUNK_ROWS)
    steps = nodes.bit_length() - 1
    chunked = (chunks, CHUNK_ROWS, width)
    dma = pltpu.SemaphoreType.DMA
    new_weights, new_residue, grad_rms = pl.pallas_call(
        partial(round_kernel, nodes, 2**level),
        out_shape=(
            jax.ShapeDtypeStruct(weights.shape, bf16),
            jax.ShapeDtypeStruct(weights.shape, bf16),
            jax.ShapeDtypeStruct((1, 8, LANES), f32),
        ),
        in_specs=[HBM] * 5,
        out_specs=(VMEM, VMEM, VMEM),
        scratch_shapes=[
            pltpu.VMEM(sample_ids.shape, jnp.int32),
            pltpu.VMEM((pool, seq, width), bf16),
            pltpu.VMEM((pool, seq, width), bf16),
            pltpu.VMEM(weights.shape[1:], bf16),
            pltpu.VMEM(weights.shape[1:], bf16),
            pltpu.VMEM((2, width, rows), bf16),
            pltpu.VMEM((3, rows, width), bf16),
            pltpu.VMEM((rows, width), f32),
            pltpu.VMEM(chunked, f32),
            pltpu.VMEM(chunked, bf16),
            pltpu.VMEM(chunked, bf16),
            pltpu.VMEM(chunked, bf16),
            pltpu.VMEM(chunked, bf16),
            pltpu.VMEM((8, width), f32),
            pltpu.VMEM((steps + 1, 8, LANES), f32),
            pltpu.VMEM((steps, 8, LANES), f32),
            dma((7 + 2 * matrices,)),
            dma((chunks,)),
            dma((chunks,)),
            dma((chunks,)),
            dma((chunks,)),
            dma((steps,)),
            dma((steps,)),
        ],
        compiler_params=pltpu.CompilerParams(
            collective_id=level, has_side_effects=True, vmem_limit_bytes=30 * 2**20
        ),
    )(sample_ids, token_pool, cotangent_pool, weights, residue)
    return new_weights, new_residue, grad_rms[0]


def write_kernel(weights_ref, residue_ref, rms_ref, weights_out, residue_out, rms_out, rms, rms_sem, sems):
    copies = []
    for n, (src, dst) in enumerate([(weights_ref, weights_out), (residue_ref, residue_out)]):
        for m in range(src.shape[1]):
            copies.append(pltpu.make_async_copy(src.at[0, m], dst.at[0, m], sems.at[n, m]))
    for copy in copies:
        copy.start()
    rms[0] = rms_ref[0, 0]
    copies.append(pltpu.make_async_copy(rms, rms_out, rms_sem))
    copies[-1].start()
    for copy in copies:
        copy.wait()


def write_out(new_weights, new_residue, grad_rms):
    shape = jax.ShapeDtypeStruct(new_weights.shape, bf16)
    dma = pltpu.SemaphoreType.DMA
    return pl.pallas_call(
        write_kernel,
        out_shape=(shape, shape, jax.ShapeDtypeStruct((1,), f32)),
        in_specs=[VMEM, VMEM, VMEM],
        out_specs=(HBM, HBM, HBM),
        scratch_shapes=[pltpu.SMEM((1,), f32), dma, dma((2, new_weights.shape[1]))],
        compiler_params=pltpu.CompilerParams(vmem_limit_bytes=8 * 2**20),
    )(new_weights, new_residue, grad_rms)


def per_device(round_index, sample_ids, token_pool, cotangent_pool, weights, residue):
    nodes = lax.axis_size("node")
    levels = nodes.bit_length() - 1
    new_weights, new_residue, grad_rms = lax.switch(
        round_index[0] % levels,
        [partial(one_round, nodes, level) for level in range(levels)],
        sample_ids,
        token_pool,
        cotangent_pool,
        weights,
        residue,
    )
    new_weights, new_residue, grad_rms = write_out(new_weights, new_residue, grad_rms)
    return (new_weights, new_residue, grad_rms[0])


def solution(mesh):
    placed = (
        P(),
        P("node", None),
        P("node", None, None, None),
        P("node", None, None, None),
        P("node", None, None, None),
        P("node", None, None, None),
    )
    return jax.shard_map(
        per_device,
        mesh=mesh,
        in_specs=placed,
        out_specs=(P("node", None, None, None), P("node", None, None, None), P()),
        check_vma=False,
    )
```

```python
from functools import partial

import jax
import jax.numpy as jnp
from jax import lax
from jax.experimental import pallas as pl
from jax.experimental.pallas import tpu as pltpu
from jax.sharding import PartitionSpec as P

HEAD_DIM = 64
LANES = 128
CHUNK_ROWS = 128
LAG = 3

epsilon = 1e-06
step_rate = 0.1

f32, bf16 = jnp.float32, jnp.bfloat16
MESH = pl.DeviceIdType.MESH
VMEM = pl.BlockSpec(memory_space=pltpu.VMEM)
HBM = pl.BlockSpec(memory_space=pltpu.HBM)


def dot(left, right, left_dim=1, right_dim=0):
    return lax.dot_general(
        left, right, (((left_dim,), (right_dim,)), ((), ())), preferred_element_type=f32
    )


def round_kernel(
    nodes,
    offset,
    ids_hbm,
    tokens_hbm,
    cot_hbm,
    weights_hbm,
    residue_hbm,
    new_weights_ref,
    new_residue_ref,
    rms_ref,
    ids_ref,
    tokens_ref,
    cot_ref,
    weights_ref,
    residue_ref,
    left_ref,
    right_ref,
    context_ref,
    gradient,
    tracked,
    tracked_in,
    sent,
    sent_in,
    squares,
    totals,
    totals_in,
    load_sems,
    track_send,
    track_recv,
    sent_send,
    sent_recv,
    sum_send,
    sum_recv,
):
    me = lax.axis_index("node")
    target = lax.rem(me + offset, nodes)
    source = lax.rem(me + nodes - offset, nodes)
    steps = nodes.bit_length() - 1
    mutual = 2 * offset == nodes
    strides = [2**k for k in range(steps)]
    if not mutual:
        strides = [offset] + [stride for stride in strides if stride != offset]
    partners = [me + stride * (1 - 2 * ((me // stride) % 2)) for stride in strides]

    pool, seq, width = tokens_ref.shape
    matrices = weights_ref.shape[0]
    rows = pool * seq
    pairs = width // LANES
    per_matrix = width // CHUNK_ROWS
    chunks = matrices * per_matrix
    proj_scale = width**-0.5
    head_scale = HEAD_DIM**-0.5
    order = [3, 2, 0, 1]

    head, rest = pl.ds(0, CHUNK_ROWS), pl.ds(CHUNK_ROWS, width - CHUNK_ROWS)
    head_cols, rest_cols = pl.ds(0, LANES), pl.ds(LANES, width - LANES)
    qkv, pair = pl.ds(0, 3), pl.ds(0, 2)
    moves = {
        "tokens": (tokens_hbm.at[0], tokens_ref),
        "w": (weights_hbm.at[0, qkv, :, head_cols], weights_ref.at[qkv, :, head_cols]),
        "ids": (ids_hbm, ids_ref),
        "cot": (cot_hbm.at[0], cot_ref),
        "r": (residue_hbm.at[0, 3, head], residue_ref.at[3, head]),
        "w+": (weights_hbm.at[0, qkv, :, rest_cols], weights_ref.at[qkv, :, rest_cols]),
        "r+": (residue_hbm.at[0, 3, rest], residue_ref.at[3, rest]),
        "w3": (weights_hbm.at[0, 3], weights_ref.at[3]),
        "r2": (residue_hbm.at[0, 2], residue_ref.at[2]),
        "r01": (residue_hbm.at[0, pair], residue_ref.at[pair]),
    }
    loads = {}
    for n, (name, move) in enumerate(moves.items()):
        loads[name] = pltpu.make_async_copy(*move, load_sems.at[n])
        loads[name].start()

    barrier = pltpu.get_barrier_semaphore()
    for other in [target, source] + partners:
        pl.semaphore_signal(barrier, inc=1, device_id=(other,), device_id_type=MESH)

    def track_copy(n, c, size=1):
        at = pl.ds(c, size)
        return pltpu.make_async_remote_copy(
            tracked.at[at],
            tracked_in.at[at],
            track_send.at[n],
            track_recv.at[c // per_matrix],
            (target,),
            MESH,
        )

    def slot(c):
        return 0 if mutual or c < per_matrix else 1 + c % per_matrix

    def sent_sem(m, c):
        first = order.index(m)
        return first if first < matrices - 1 else c - first * (per_matrix - 1)

    def sent_copy(m, c):
        return pltpu.make_async_remote_copy(
            sent.at[c], sent_in.at[c], sent_send.at[0], sent_recv.at[sent_sem(m, c)], (target,), MESH
        )

    def weights_copy(m, part, c):
        return pltpu.make_async_remote_copy(
            weights_hbm.at[0, m, part],
            sent_in.at[c],
            sent_send.at[0],
            sent_recv.at[sent_sem(m, c)],
            (target,),
            MESH,
        )

    def sent_span(c, size, sem):
        at = pl.ds(c, size)
        return pltpu.make_async_remote_copy(
            sent.at[at], sent_in.at[at], sent_send.at[0], sent_recv.at[sem], (target,), MESH
        )

    def await_tracked(m):
        track_copy(0, order.index(m) * per_matrix, per_matrix).wait_recv()

    def await_sent(m):
        first = order.index(m)
        if first < matrices - 1:
            sent_span(first * per_matrix, per_matrix, first).wait_recv()

    def await_last(m, c):
        if order.index(m) == matrices - 1:
            sent_span(c, 1, sent_sem(m, c)).wait_recv()

    def each_block(which, body):
        for m in which:

            @pl.loop(0, per_matrix)
            def _(r):
                body(m, pl.ds(r * CHUNK_ROWS, CHUNK_ROWS), order.index(m) * per_matrix + r)

    def send_weights(m, part, c):
        weights_copy(m, part, c).start()

    if mutual:
        pl.semaphore_wait(barrier, 2 + steps)
        each_block(order[:2], send_weights)

    loads["tokens"].wait()
    values = tokens_ref[...].reshape(rows, width).astype(f32)
    centered = values - jnp.mean(values, -1, keepdims=True)
    variance = jnp.mean(centered * centered, -1, keepdims=True)
    unit_rows = centered * lax.rsqrt(variance + epsilon)
    normed = unit_rows.astype(bf16)
    first = lax.broadcasted_iota(jnp.int32, (seq, LANES), 1) < HEAD_DIM
    units = [(i, j) for i in range(pool) for j in range(pairs)]
    spots = [
        (slice(i * seq, (i + 1) * seq), slice(j * LANES, (j + 1) * LANES)) for i, j in units
    ]

    def spread(block):
        zero = jnp.zeros_like(block)
        return jnp.concatenate([jnp.where(first, block, zero), jnp.where(first, zero, block)], 0)

    def gather(block):
        return jnp.where(first, block[:seq], block[seq:])

    def track(m, part, c):
        right = right_ref[m] if m < 3 else cot
        grad = dot(left_ref[m // 3, part], right) * proj_scale
        gradient[c] = grad
        tracked[c] = (residue_ref[m, part].astype(f32) + grad).astype(bf16)
        if mutual or m == order[0]:
            track_copy(0, c).start()
        elif m == order[1]:
            track_copy(1 + c - per_matrix, c).start()
        squares[...] += jnp.sum((grad * grad).reshape(-1, 8, width), 0)

    loads["ids"].wait()
    ids = ids_ref[...]
    counts = [jnp.sum((ids == image).astype(f32), 1, keepdims=True) for image in range(pool)]
    loads["cot"].wait()
    cot = cot_ref[...].reshape(rows, width)
    squares[...] = jnp.zeros_like(squares)
    queries2, keys1, vals1, probs, half = {}, {}, {}, {}, {}
    for j in range(pairs):
        cols = slice(j * LANES, (j + 1) * LANES)
        if j < 2:
            loads["w+" if j else "w"].wait()
        queries, keys, vals = [
            (dot(normed, weights_ref[m, :, cols]) * proj_scale).astype(bf16) for m in range(3)
        ]
        here = [(i, j) for i in range(pool)]
        for i, u in enumerate(here):
            part = slice(i * seq, (i + 1) * seq)
            queries2[u], keys1[u], vals1[u] = spread(queries[part]), keys[part], vals[part]
        scores = [dot(queries2[u], keys1[u], 1, 1) * head_scale for u in here]
        for u, score in zip(here, scores):
            e = jnp.exp(score - jnp.max(score, -1, keepdims=True))
            probs[u] = e / jnp.sum(e, -1, keepdims=True)
            half[u] = probs[u].astype(bf16)
        context = [gather(dot(half[u], vals1[u])) * counts[u[0]] for u in here]
        left_ref[1, cols] = jnp.concatenate(context, 0).T.astype(bf16)
        if j == 0 and not mutual:
            pl.semaphore_wait(barrier, 2 + steps)
        if j < 2:
            loads["r+" if j else "r"].wait()
        track(3, pl.ds(j * LANES, LANES), order.index(3) * per_matrix + j)

    loads["w3"].wait()
    context_grad = (dot(cot, weights_ref[3], 1, 1) * proj_scale).astype(bf16)
    weighted = [unit_rows[i * seq : (i + 1) * seq] * counts[i] for i in range(pool)]
    left_ref[0] = jnp.concatenate(weighted, 0).T.astype(bf16)
    queries2, keys1, vals1, probs, half = [
        [found[u] for u in units] for found in (queries2, keys1, vals1, probs, half)
    ]
    grads2 = [spread(context_grad[at]) for at in spots]
    for n, at in enumerate(spots):
        right_ref[2, at[0], at[1]] = dot(half[n], grads2[n], 0, 0).astype(bf16)
    loads["r2"].wait()
    each_block([2], track)
    probs_grad = [dot(g, v, 1, 1) for g, v in zip(grads2, vals1)]
    score_grad = []
    for p, g in zip(probs, probs_grad):
        inner = jnp.sum(g * p, -1, keepdims=True)
        score_grad.append((p * (g - inner) * head_scale).astype(bf16))
    for n, at in enumerate(spots):
        right_ref[0, at[0], at[1]] = gather(dot(score_grad[n], keys1[n])).astype(bf16)
        right_ref[1, at[0], at[1]] = dot(score_grad[n], queries2[n], 0, 0).astype(bf16)
    loads["r01"].wait()
    each_block(order[2:], track)

    def sum_copy(k):
        return pltpu.make_async_remote_copy(
            totals.at[k], totals_in.at[k], sum_send.at[0], sum_recv.at[k], (partners[k],), MESH
        )

    def sum_finish(k):
        sum_copy(k).wait()
        totals[k + 1] = totals[k] + totals_in[k]

    own_total = jnp.sum(jnp.sum(squares[...], 0, keepdims=True), 1, keepdims=True)
    totals[0] = jnp.broadcast_to(own_total, totals.shape[1:])
    entries = nodes * matrices * width * width

    def set_rms():
        rms_ref[0] = jnp.sqrt(totals[steps] / entries)

    def mix(m, part, c):
        tracker = 0.5 * (tracked[c].astype(f32) + tracked_in[c].astype(f32))
        own = weights_ref[m, part].astype(f32)
        new_residue_ref[0, m, part] = (tracker - gradient[c]).astype(bf16)
        base = 0.5 * own - 0.5 * step_rate * tracker
        if mutual:
            await_last(m, c)
            peer_sent = (sent_in[c].astype(f32) - step_rate * tracker).astype(bf16)
            new_weights_ref[0, m, part] = (base + 0.5 * peer_sent.astype(f32)).astype(bf16)
        else:
            sent[c] = (own - step_rate * tracker).astype(bf16)
            sent_copy(m, c).start()
            gradient[c] = base

    def mix_all(which):
        for m in which:
            await_tracked(m)
            if mutual:
                await_sent(m)
            each_block([m], mix)

    def finish(m, part, c):
        await_last(m, c)
        new_weights_ref[0, m, part] = (gradient[c] + 0.5 * sent_in[c].astype(f32)).astype(bf16)

    if mutual:
        for k in range(steps - 2):
            sum_copy(k).start()
            sum_finish(k)
        for n, k in enumerate([steps - 2, steps - 1]):
            sum_copy(k).start()
            each_block([order[2 + n]], send_weights)
            mix_all([order[n]])
            sum_finish(k)
        set_rms()
        mix_all(order[2:])
        track_copy(0, 0, chunks).wait_send()
    else:
        held = 2 * per_matrix
        starts = [held + k * (chunks - held) // steps for k in range(steps)]
        gone = per_matrix
        for c in range(held, chunks):
            while gone <= c - LAG:
                track_copy(slot(gone), gone).wait_send()
                gone += 1
            for k in range(steps):
                if starts[k] == c:
                    if k:
                        sum_finish(k - 1)
                    sum_copy(k).start()
            track_copy(slot(c), c).start()
        sum_finish(steps - 1)
        set_rms()
        mix_all(order)
        for m in order:
            await_sent(m)
            each_block([m], finish)
        track_copy(0, 0, per_matrix).wait_send()
        for c in range(gone, chunks):
            track_copy(slot(c), c).wait_send()
    sent_span(0, chunks, 0).wait_send()


def one_round(nodes, level, sample_ids, token_pool, cotangent_pool, weights, residue):
    pool, seq, width = token_pool.shape[1:]
    matrices = weights.shape[1]
    rows = pool * seq
    per_matrix = width // CHUNK_ROWS
    chunks = matrices * per_matrix
    steps = nodes.bit_length() - 1
    chunked = (chunks, CHUNK_ROWS, width)
    dma = pltpu.SemaphoreType.DMA
    new_weights, new_residue, grad_rms = pl.pallas_call(
        partial(round_kernel, nodes, 2**level),
        out_shape=(
            jax.ShapeDtypeStruct(weights.shape, bf16),
            jax.ShapeDtypeStruct(weights.shape, bf16),
            jax.ShapeDtypeStruct((1, 8, LANES), f32),
        ),
        in_specs=[HBM] * 5,
        out_specs=(VMEM, VMEM, VMEM),
        scratch_shapes=[
            pltpu.VMEM(sample_ids.shape, jnp.int32),
            pltpu.VMEM((pool, seq, width), bf16),
            pltpu.VMEM((pool, seq, width), bf16),
            pltpu.VMEM(weights.shape[1:], bf16),
            pltpu.VMEM(weights.shape[1:], bf16),
            pltpu.VMEM((2, width, rows), bf16),
            pltpu.VMEM((3, rows, width), bf16),
            pltpu.VMEM((rows, width), f32),
            pltpu.VMEM(chunked, f32),
            pltpu.VMEM(chunked, bf16),
            pltpu.VMEM(chunked, bf16),
            pltpu.VMEM(chunked, bf16),
            pltpu.VMEM(chunked, bf16),
            pltpu.VMEM((8, width), f32),
            pltpu.VMEM((steps + 1, 8, LANES), f32),
            pltpu.VMEM((steps, 8, LANES), f32),
            dma((10,)),
            dma((1 + per_matrix,)),
            dma((matrices,)),
            dma((1,)),
            dma((matrices - 1 + per_matrix,)),
            dma((1,)),
            dma((steps,)),
        ],
        compiler_params=pltpu.CompilerParams(
            collective_id=level, has_side_effects=True, vmem_limit_bytes=30 * 2**20
        ),
    )(sample_ids, token_pool, cotangent_pool, weights, residue)
    return new_weights, new_residue, grad_rms[0]


def write_kernel(weights_ref, residue_ref, rms_ref, weights_out, residue_out, rms_out, rms, rms_sem, sems):
    copies = []
    for n, (src, dst) in enumerate([(weights_ref, weights_out), (residue_ref, residue_out)]):
        for m in range(src.shape[1]):
            copies.append(pltpu.make_async_copy(src.at[0, m], dst.at[0, m], sems.at[n, m]))
    for copy in copies:
        copy.start()
    rms[0] = rms_ref[0, 0]
    copies.append(pltpu.make_async_copy(rms, rms_out, rms_sem))
    copies[-1].start()
    for copy in copies:
        copy.wait()


def write_out(new_weights, new_residue, grad_rms):
    shape = jax.ShapeDtypeStruct(new_weights.shape, bf16)
    dma = pltpu.SemaphoreType.DMA
    return pl.pallas_call(
        write_kernel,
        out_shape=(shape, shape, jax.ShapeDtypeStruct((1,), f32)),
        in_specs=[VMEM, VMEM, VMEM],
        out_specs=(HBM, HBM, HBM),
        scratch_shapes=[pltpu.SMEM((1,), f32), dma, dma((2, new_weights.shape[1]))],
        compiler_params=pltpu.CompilerParams(vmem_limit_bytes=8 * 2**20),
    )(new_weights, new_residue, grad_rms)


def per_device(round_index, sample_ids, token_pool, cotangent_pool, weights, residue):
    nodes = lax.axis_size("node")
    levels = nodes.bit_length() - 1
    new_weights, new_residue, grad_rms = lax.switch(
        round_index[0] % levels,
        [partial(one_round, nodes, level) for level in range(levels)],
        sample_ids,
        token_pool,
        cotangent_pool,
        weights,
        residue,
    )
    new_weights, new_residue, grad_rms = write_out(new_weights, new_residue, grad_rms)
    return (new_weights, new_residue, grad_rms[0])


def solution(mesh):
    placed = (
        P(),
        P("node", None),
        P("node", None, None, None),
        P("node", None, None, None),
        P("node", None, None, None),
        P("node", None, None, None),
    )
    return jax.shard_map(
        per_device,
        mesh=mesh,
        in_specs=placed,
        out_specs=(P("node", None, None, None), P("node", None, None, None), P()),
        check_vma=False,
    )
```

```python
from functools import partial

import jax
import jax.numpy as jnp
from jax import lax
from jax.experimental import pallas as pl
from jax.experimental.pallas import tpu as pltpu
from jax.sharding import PartitionSpec as P

HEAD_DIM = 64
LANES = 128
CHUNK_ROWS = 128
LAG = 3

epsilon = 1e-06
step_rate = 0.1

f32, bf16 = jnp.float32, jnp.bfloat16
MESH = pl.DeviceIdType.MESH
VMEM = pl.BlockSpec(memory_space=pltpu.VMEM)
HBM = pl.BlockSpec(memory_space=pltpu.HBM)


def dot(left, right, left_dim=1, right_dim=0):
    return lax.dot_general(
        left, right, (((left_dim,), (right_dim,)), ((), ())), preferred_element_type=f32
    )


def round_kernel(
    nodes,
    offset,
    ids_hbm,
    tokens_hbm,
    cot_hbm,
    weights_hbm,
    residue_hbm,
    new_weights_ref,
    new_residue_ref,
    rms_ref,
    ids_ref,
    tokens_ref,
    cot_ref,
    weights_ref,
    residue_ref,
    left_ref,
    right_ref,
    context_ref,
    gradient,
    tracked,
    tracked_in,
    sent,
    sent_in,
    squares,
    totals,
    totals_in,
    load_sems,
    track_send,
    track_recv,
    sent_send,
    sent_recv,
    sum_send,
    sum_recv,
):
    me = lax.axis_index("node")
    target = lax.rem(me + offset, nodes)
    source = lax.rem(me + nodes - offset, nodes)
    steps = nodes.bit_length() - 1
    mutual = 2 * offset == nodes
    strides = [2**k for k in range(steps)]
    if not mutual:
        strides = [offset] + [stride for stride in strides if stride != offset]
    partners = [me + stride * (1 - 2 * ((me // stride) % 2)) for stride in strides]

    pool, seq, width = tokens_ref.shape
    matrices = weights_ref.shape[0]
    rows = pool * seq
    pairs = width // LANES
    per_matrix = width // CHUNK_ROWS
    chunks = matrices * per_matrix
    proj_scale = width**-0.5
    head_scale = HEAD_DIM**-0.5
    order = [3, 2, 0, 1]

    head, rest = pl.ds(0, CHUNK_ROWS), pl.ds(CHUNK_ROWS, width - CHUNK_ROWS)
    head_cols, rest_cols = pl.ds(0, LANES), pl.ds(LANES, width - LANES)
    qkv, pair = pl.ds(0, 3), pl.ds(0, 2)
    moves = {
        "tokens": (tokens_hbm.at[0], tokens_ref),
        "w": (weights_hbm.at[0, qkv, :, head_cols], weights_ref.at[qkv, :, head_cols]),
        "ids": (ids_hbm, ids_ref),
        "cot": (cot_hbm.at[0], cot_ref),
        "r": (residue_hbm.at[0, 3, head], residue_ref.at[3, head]),
        "w+": (weights_hbm.at[0, qkv, :, rest_cols], weights_ref.at[qkv, :, rest_cols]),
        "r+": (residue_hbm.at[0, 3, rest], residue_ref.at[3, rest]),
        "w3": (weights_hbm.at[0, 3], weights_ref.at[3]),
        "r2": (residue_hbm.at[0, 2], residue_ref.at[2]),
        "r01": (residue_hbm.at[0, pair], residue_ref.at[pair]),
    }
    loads = {}
    for n, (name, move) in enumerate(moves.items()):
        loads[name] = pltpu.make_async_copy(*move, load_sems.at[n])
        loads[name].start()

    barrier = pltpu.get_barrier_semaphore()
    for other in [target, source] + partners:
        pl.semaphore_signal(barrier, inc=1, device_id=(other,), device_id_type=MESH)

    def track_copy(n, c, size=1):
        at = pl.ds(c, size)
        return pltpu.make_async_remote_copy(
            tracked.at[at],
            tracked_in.at[at],
            track_send.at[n],
            track_recv.at[c // per_matrix],
            (target,),
            MESH,
        )

    def slot(c):
        return 0 if mutual or c < per_matrix else 1 + c % per_matrix

    def sent_sem(m, c):
        first = order.index(m)
        return first if first < matrices - 1 else c - first * (per_matrix - 1)

    def sent_copy(m, c):
        return pltpu.make_async_remote_copy(
            sent.at[c], sent_in.at[c], sent_send.at[0], sent_recv.at[sent_sem(m, c)], (target,), MESH
        )

    def weights_copy(m, part, c):
        return pltpu.make_async_remote_copy(
            weights_hbm.at[0, m, part],
            sent_in.at[c],
            sent_send.at[0],
            sent_recv.at[sent_sem(m, c)],
            (target,),
            MESH,
        )

    def sent_span(c, size, sem):
        at = pl.ds(c, size)
        return pltpu.make_async_remote_copy(
            sent.at[at], sent_in.at[at], sent_send.at[0], sent_recv.at[sem], (target,), MESH
        )

    def await_tracked(m):
        track_copy(0, order.index(m) * per_matrix, per_matrix).wait_recv()

    def await_sent(m):
        first = order.index(m)
        if first < matrices - 1:
            sent_span(first * per_matrix, per_matrix, first).wait_recv()

    def await_last(m, c):
        if order.index(m) == matrices - 1:
            sent_span(c, 1, sent_sem(m, c)).wait_recv()

    def each_block(which, body):
        for m in which:

            @pl.loop(0, per_matrix)
            def _(r):
                body(m, pl.ds(r * CHUNK_ROWS, CHUNK_ROWS), order.index(m) * per_matrix + r)

    def send_weights(m, part, c):
        weights_copy(m, part, c).start()

    if mutual:
        pl.semaphore_wait(barrier, 2 + steps)
        each_block(order[:2], send_weights)

    loads["tokens"].wait()
    values = tokens_ref[...].reshape(rows, width).astype(f32)
    centered = values - jnp.mean(values, -1, keepdims=True)
    variance = jnp.mean(centered * centered, -1, keepdims=True)
    unit_rows = centered * lax.rsqrt(variance + epsilon)
    normed = unit_rows.astype(bf16)
    first = lax.broadcasted_iota(jnp.int32, (seq, LANES), 1) < HEAD_DIM
    units = [(i, j) for i in range(pool) for j in range(pairs)]
    spots = [
        (slice(i * seq, (i + 1) * seq), slice(j * LANES, (j + 1) * LANES)) for i, j in units
    ]

    def spread(block):
        zero = jnp.zeros_like(block)
        return jnp.concatenate([jnp.where(first, block, zero), jnp.where(first, zero, block)], 0)

    def gather(block):
        return jnp.where(first, block[:seq], block[seq:])

    def track(m, part, c):
        right = right_ref[m] if m < 3 else cot
        grad = dot(left_ref[m // 3, part], right) * proj_scale
        gradient[c] = grad
        tracked[c] = (residue_ref[m, part].astype(f32) + grad).astype(bf16)
        if mutual or m == order[0]:
            track_copy(0, c).start()
        elif m == order[1]:
            track_copy(1 + c - per_matrix, c).start()
        squares[...] += jnp.sum((grad * grad).reshape(-1, 8, width), 0)

    loads["ids"].wait()
    ids = ids_ref[...]
    counts = [jnp.sum((ids == image).astype(f32), 1, keepdims=True) for image in range(pool)]
    loads["cot"].wait()
    cot = cot_ref[...].reshape(rows, width)
    squares[...] = jnp.zeros_like(squares)
    queries2, keys1, vals1, probs, half = {}, {}, {}, {}, {}
    for j in range(pairs):
        cols = slice(j * LANES, (j + 1) * LANES)
        if j < 2:
            loads["w+" if j else "w"].wait()
        queries, keys, vals = [
            (dot(normed, weights_ref[m, :, cols]) * proj_scale).astype(bf16) for m in range(3)
        ]
        here = [(i, j) for i in range(pool)]
        for i, u in enumerate(here):
            part = slice(i * seq, (i + 1) * seq)
            queries2[u], keys1[u], vals1[u] = spread(queries[part]), keys[part], vals[part]
        scores = [dot(queries2[u], keys1[u], 1, 1) * head_scale for u in here]
        for u, score in zip(here, scores):
            e = jnp.exp(score - jnp.max(score, -1, keepdims=True))
            probs[u] = e / jnp.sum(e, -1, keepdims=True)
            half[u] = probs[u].astype(bf16)
        context = [gather(dot(half[u], vals1[u])) * counts[u[0]] for u in here]
        left_ref[1, cols] = jnp.concatenate(context, 0).T.astype(bf16)
        if j == 0 and not mutual:
            pl.semaphore_wait(barrier, 2 + steps)
        if j < 2:
            loads["r+" if j else "r"].wait()
        track(3, pl.ds(j * LANES, LANES), order.index(3) * per_matrix + j)

    loads["w3"].wait()
    context_grad = (dot(cot, weights_ref[3], 1, 1) * proj_scale).astype(bf16)
    weighted = [unit_rows[i * seq : (i + 1) * seq] * counts[i] for i in range(pool)]
    left_ref[0] = jnp.concatenate(weighted, 0).T.astype(bf16)
    queries2, keys1, vals1, probs, half = [
        [found[u] for u in units] for found in (queries2, keys1, vals1, probs, half)
    ]
    grads2 = [spread(context_grad[at]) for at in spots]
    for n, at in enumerate(spots):
        right_ref[2, at[0], at[1]] = dot(half[n], grads2[n], 0, 0).astype(bf16)
    loads["r2"].wait()
    each_block([2], track)
    probs_grad = [dot(g, v, 1, 1) for g, v in zip(grads2, vals1)]
    score_grad = []
    for p, g in zip(probs, probs_grad):
        inner = jnp.sum(g * p, -1, keepdims=True)
        score_grad.append((p * (g - inner) * head_scale).astype(bf16))
    for n, at in enumerate(spots):
        right_ref[0, at[0], at[1]] = gather(dot(score_grad[n], keys1[n])).astype(bf16)
        right_ref[1, at[0], at[1]] = dot(score_grad[n], queries2[n], 0, 0).astype(bf16)
    loads["r01"].wait()
    each_block(order[2:], track)

    def sum_copy(k):
        return pltpu.make_async_remote_copy(
            totals.at[k], totals_in.at[k], sum_send.at[0], sum_recv.at[k], (partners[k],), MESH
        )

    def sum_finish(k):
        sum_copy(k).wait()
        totals[k + 1] = totals[k] + totals_in[k]

    own_total = jnp.sum(jnp.sum(squares[...], 0, keepdims=True), 1, keepdims=True)
    totals[0] = jnp.broadcast_to(own_total, totals.shape[1:])
    entries = nodes * matrices * width * width

    def set_rms():
        rms_ref[0] = jnp.sqrt(totals[steps] / entries)

    def mix(m, part, c):
        tracker = 0.5 * (tracked[c].astype(f32) + tracked_in[c].astype(f32))
        own = weights_ref[m, part].astype(f32)
        new_residue_ref[0, m, part] = (tracker - gradient[c]).astype(bf16)
        base = 0.5 * own - 0.5 * step_rate * tracker
        if mutual:
            await_last(m, c)
            peer_sent = (sent_in[c].astype(f32) - step_rate * tracker).astype(bf16)
            new_weights_ref[0, m, part] = (base + 0.5 * peer_sent.astype(f32)).astype(bf16)
        else:
            sent[c] = (own - step_rate * tracker).astype(bf16)
            sent_copy(m, c).start()
            gradient[c] = base

    def mix_all(which):
        for m in which:
            await_tracked(m)
            if mutual:
                await_sent(m)
            each_block([m], mix)

    def finish(m, part, c):
        await_last(m, c)
        new_weights_ref[0, m, part] = (gradient[c] + 0.5 * sent_in[c].astype(f32)).astype(bf16)

    if mutual:
        for k in range(steps - 2):
            sum_copy(k).start()
            sum_finish(k)
        for n, k in enumerate([steps - 2, steps - 1]):
            sum_copy(k).start()
            each_block([order[2 + n]], send_weights)
            mix_all([order[n]])
            sum_finish(k)
        set_rms()
        mix_all(order[2:])
        track_copy(0, 0, chunks).wait_send()
    else:
        held = 2 * per_matrix
        starts = [held + k * (chunks - held) // steps for k in range(steps)]

        def hand_out(lag):
            gone = per_matrix
            for c in range(held, chunks):
                while gone <= c - (lag if c >= chunks - per_matrix else LAG):
                    track_copy(slot(gone), gone).wait_send()
                    gone += 1
                for k in range(steps):
                    if starts[k] == c:
                        if k:
                            sum_finish(k - 1)
                        sum_copy(k).start()
                track_copy(slot(c), c).start()
        if offset == 1:
            hand_out(LAG)
        else:
            @pl.when(me % 2 == 0)
            def _():
                hand_out(LAG)

            @pl.when(me % 2 == 1)
            def _():
                hand_out(1)

        sum_finish(steps - 1)
        set_rms()
        mix_all(order)
        for m in order:
            await_sent(m)
            each_block([m], finish)
        track_copy(0, 0, per_matrix).wait_send()

        def await_gone(lag):
            for c in range(chunks - lag, chunks):
                track_copy(slot(c), c).wait_send()

        if offset == 1:
            await_gone(LAG)
        else:
            pl.when(me % 2 == 0)(lambda: await_gone(LAG))
            pl.when(me % 2 == 1)(lambda: await_gone(1))
    sent_span(0, chunks, 0).wait_send()


def one_round(nodes, level, sample_ids, token_pool, cotangent_pool, weights, residue):
    pool, seq, width = token_pool.shape[1:]
    matrices = weights.shape[1]
    rows = pool * seq
    per_matrix = width // CHUNK_ROWS
    chunks = matrices * per_matrix
    steps = nodes.bit_length() - 1
    chunked = (chunks, CHUNK_ROWS, width)
    dma = pltpu.SemaphoreType.DMA
    new_weights, new_residue, grad_rms = pl.pallas_call(
        partial(round_kernel, nodes, 2**level),
        out_shape=(
            jax.ShapeDtypeStruct(weights.shape, bf16),
            jax.ShapeDtypeStruct(weights.shape, bf16),
            jax.ShapeDtypeStruct((1, 8, LANES), f32),
        ),
        in_specs=[HBM] * 5,
        out_specs=(VMEM, VMEM, VMEM),
        scratch_shapes=[
            pltpu.VMEM(sample_ids.shape, jnp.int32),
            pltpu.VMEM((pool, seq, width), bf16),
            pltpu.VMEM((pool, seq, width), bf16),
            pltpu.VMEM(weights.shape[1:], bf16),
            pltpu.VMEM(weights.shape[1:], bf16),
            pltpu.VMEM((2, width, rows), bf16),
            pltpu.VMEM((3, rows, width), bf16),
            pltpu.VMEM((rows, width), f32),
            pltpu.VMEM(chunked, f32),
            pltpu.VMEM(chunked, bf16),
            pltpu.VMEM(chunked, bf16),
            pltpu.VMEM(chunked, bf16),
            pltpu.VMEM(chunked, bf16),
            pltpu.VMEM((8, width), f32),
            pltpu.VMEM((steps + 1, 8, LANES), f32),
            pltpu.VMEM((steps, 8, LANES), f32),
            dma((10,)),
            dma((1 + per_matrix,)),
            dma((matrices,)),
            dma((1,)),
            dma((matrices - 1 + per_matrix,)),
            dma((1,)),
            dma((steps,)),
        ],
        compiler_params=pltpu.CompilerParams(
            collective_id=level, has_side_effects=True, vmem_limit_bytes=30 * 2**20
        ),
    )(sample_ids, token_pool, cotangent_pool, weights, residue)
    return new_weights, new_residue, grad_rms[0]


def write_kernel(weights_ref, residue_ref, rms_ref, weights_out, residue_out, rms_out, rms, rms_sem, sems):
    copies = []
    for n, (src, dst) in enumerate([(weights_ref, weights_out), (residue_ref, residue_out)]):
        for m in range(src.shape[1]):
            copies.append(pltpu.make_async_copy(src.at[0, m], dst.at[0, m], sems.at[n, m]))
    for copy in copies:
        copy.start()
    rms[0] = rms_ref[0, 0]
    copies.append(pltpu.make_async_copy(rms, rms_out, rms_sem))
    copies[-1].start()
    for copy in copies:
        copy.wait()


def write_out(new_weights, new_residue, grad_rms):
    shape = jax.ShapeDtypeStruct(new_weights.shape, bf16)
    dma = pltpu.SemaphoreType.DMA
    return pl.pallas_call(
        write_kernel,
        out_shape=(shape, shape, jax.ShapeDtypeStruct((1,), f32)),
        in_specs=[VMEM, VMEM, VMEM],
        out_specs=(HBM, HBM, HBM),
        scratch_shapes=[pltpu.SMEM((1,), f32), dma, dma((2, new_weights.shape[1]))],
        compiler_params=pltpu.CompilerParams(vmem_limit_bytes=8 * 2**20),
    )(new_weights, new_residue, grad_rms)


def per_device(round_index, sample_ids, token_pool, cotangent_pool, weights, residue):
    nodes = lax.axis_size("node")
    levels = nodes.bit_length() - 1
    new_weights, new_residue, grad_rms = lax.switch(
        round_index[0] % levels,
        [partial(one_round, nodes, level) for level in range(levels)],
        sample_ids,
        token_pool,
        cotangent_pool,
        weights,
        residue,
    )
    new_weights, new_residue, grad_rms = write_out(new_weights, new_residue, grad_rms)
    return (new_weights, new_residue, grad_rms[0])


def solution(mesh):
    placed = (
        P(),
        P("node", None),
        P("node", None, None, None),
        P("node", None, None, None),
        P("node", None, None, None),
        P("node", None, None, None),
    )
    return jax.shard_map(
        per_device,
        mesh=mesh,
        in_specs=placed,
        out_specs=(P("node", None, None, None), P("node", None, None, None), P()),
        check_vma=False,
    )
```

```python
from functools import partial

import jax
import jax.numpy as jnp
from jax import lax
from jax.experimental import pallas as pl
from jax.experimental.pallas import tpu as pltpu
from jax.sharding import PartitionSpec as P

HEAD_DIM = 64
LANES = 128
CHUNK_ROWS = 128
LAG = 3

epsilon = 1e-06
step_rate = 0.1

f32, bf16 = jnp.float32, jnp.bfloat16
MESH = pl.DeviceIdType.MESH
VMEM = pl.BlockSpec(memory_space=pltpu.VMEM)
HBM = pl.BlockSpec(memory_space=pltpu.HBM)


def dot(left, right, left_dim=1, right_dim=0):
    return lax.dot_general(
        left, right, (((left_dim,), (right_dim,)), ((), ())), preferred_element_type=f32
    )


def round_kernel(
    nodes,
    offset,
    ids_hbm,
    tokens_hbm,
    cot_hbm,
    weights_hbm,
    residue_hbm,
    new_weights_ref,
    new_residue_ref,
    rms_ref,
    ids_ref,
    tokens_ref,
    cot_ref,
    weights_ref,
    residue_ref,
    left_ref,
    right_ref,
    context_ref,
    gradient,
    tracked,
    tracked_in,
    sent,
    sent_in,
    squares,
    totals,
    totals_in,
    load_sems,
    track_send,
    track_recv,
    sent_send,
    sent_recv,
    sum_send,
    sum_recv,
):
    me = lax.axis_index("node")
    target = lax.rem(me + offset, nodes)
    source = lax.rem(me + nodes - offset, nodes)
    steps = nodes.bit_length() - 1
    mutual = 2 * offset == nodes
    strides = [2**k for k in range(steps)]
    if not mutual:
        strides = [offset] + [stride for stride in strides if stride != offset]
    partners = [me + stride * (1 - 2 * ((me // stride) % 2)) for stride in strides]

    pool, seq, width = tokens_ref.shape
    matrices = weights_ref.shape[0]
    rows = pool * seq
    pairs = width // LANES
    per_matrix = width // CHUNK_ROWS
    chunks = matrices * per_matrix
    proj_scale = width**-0.5
    head_scale = HEAD_DIM**-0.5
    last = matrices - 1
    tail = last * per_matrix

    head, rest = pl.ds(0, CHUNK_ROWS), pl.ds(CHUNK_ROWS, width - CHUNK_ROWS)
    head_cols, rest_cols = pl.ds(0, LANES), pl.ds(LANES, width - LANES)
    qkv, pair = pl.ds(0, 3), pl.ds(0, 2)
    moves = {
        "tokens": (tokens_hbm.at[0], tokens_ref),
        "w": (weights_hbm.at[0, qkv, :, head_cols], weights_ref.at[qkv, :, head_cols]),
        "ids": (ids_hbm, ids_ref),
        "cot": (cot_hbm.at[0], cot_ref),
        "r": (residue_hbm.at[0, 3, head], residue_ref.at[3, head]),
        "w+": (weights_hbm.at[0, qkv, :, rest_cols], weights_ref.at[qkv, :, rest_cols]),
        "r+": (residue_hbm.at[0, 3, rest], residue_ref.at[3, rest]),
        "w3": (weights_hbm.at[0, 3], weights_ref.at[3]),
        "r2": (residue_hbm.at[0, 2], residue_ref.at[2]),
        "r01": (residue_hbm.at[0, pair], residue_ref.at[pair]),
    }
    loads = {}
    for n, (name, move) in enumerate(moves.items()):
        loads[name] = pltpu.make_async_copy(*move, load_sems.at[n])
        loads[name].start()

    barrier = pltpu.get_barrier_semaphore()
    for other in [target, source] + partners:
        pl.semaphore_signal(barrier, inc=1, device_id=(other,), device_id_type=MESH)

    def track_copy(n, c, size=1):
        at = pl.ds(c, size)
        return pltpu.make_async_remote_copy(
            tracked.at[at],
            tracked_in.at[at],
            track_send.at[n],
            track_recv.at[c // per_matrix],
            (target,),
            MESH,
        )

    def slot(c):
        return 0 if mutual else 1 + c % per_matrix

    def sent_sem(c):
        return c // per_matrix + (c % per_matrix) * (c // tail)

    def sent_copy(c, size=1):
        at = pl.ds(c, size)
        return pltpu.make_async_remote_copy(
            sent.at[at], sent_in.at[at], sent_send.at[0], sent_recv.at[sent_sem(c)], (target,), MESH
        )

    def send_weights(m, part, c):
        pltpu.make_async_remote_copy(
            weights_hbm.at[0, m, part],
            sent_in.at[c],
            sent_send.at[0],
            sent_recv.at[sent_sem(c)],
            (target,),
            MESH,
        ).start()

    def await_sent(c):
        @pl.when(c >= tail)
        def _():
            sent_copy(c).wait_recv()

        @pl.when((c < tail) & (c % per_matrix == 0))
        def _():
            sent_copy(c, per_matrix).wait_recv()

    def each_block(first, end, body):
        @pl.loop(first * per_matrix, end * per_matrix)
        def _(c):
            body(last - c // per_matrix, pl.ds((c % per_matrix) * CHUNK_ROWS, CHUNK_ROWS), c)

    if mutual:
        pl.semaphore_wait(barrier, 2 + steps)
        each_block(0, 2, send_weights)

    loads["tokens"].wait()
    values = tokens_ref[...].reshape(rows, width).astype(f32)
    centered = values - jnp.mean(values, -1, keepdims=True)
    variance = jnp.mean(centered * centered, -1, keepdims=True)
    unit_rows = centered * lax.rsqrt(variance + epsilon)
    normed = unit_rows.astype(bf16)
    first = lax.broadcasted_iota(jnp.int32, (seq, LANES), 1) < HEAD_DIM
    units = [(i, j) for i in range(pool) for j in range(pairs)]
    spots = [
        (slice(i * seq, (i + 1) * seq), slice(j * LANES, (j + 1) * LANES)) for i, j in units
    ]

    def spread(block):
        zero = jnp.zeros_like(block)
        return jnp.concatenate([jnp.where(first, block, zero), jnp.where(first, zero, block)], 0)

    def gather(block):
        return jnp.where(first, block[:seq], block[seq:])

    def track(left, right, m, part, c):
        grad = dot(left, right) * proj_scale
        gradient[c] = grad
        tracked[c] = (residue_ref[m, part].astype(f32) + grad).astype(bf16)
        squares[...] += jnp.sum((grad * grad).reshape(-1, 8, width), 0)

    def track_value(m, part, c):
        track(left_ref[0, part], right_ref[2], m, part, c)
        track_copy(slot(c), c).start()

    def track_rest(m, part, c):
        track(left_ref[0, part], right_ref[m], m, part, c)
        if mutual:
            track_copy(slot(c), c).start()

    loads["ids"].wait()
    ids = ids_ref[...]
    counts = [jnp.sum((ids == image).astype(f32), 1, keepdims=True) for image in range(pool)]
    loads["cot"].wait()
    cot = cot_ref[...].reshape(rows, width)
    squares[...] = jnp.zeros_like(squares)
    queries2, keys1, vals1, probs, half = {}, {}, {}, {}, {}
    for j in range(pairs):
        cols = slice(j * LANES, (j + 1) * LANES)
        if j < 2:
            loads["w+" if j else "w"].wait()
            loads["r+" if j else "r"].wait()
        queries, keys, vals = [
            (dot(normed, weights_ref[m, :, cols]) * proj_scale).astype(bf16) for m in range(3)
        ]
        here = [(i, j) for i in range(pool)]
        for i, u in enumerate(here):
            part = slice(i * seq, (i + 1) * seq)
            queries2[u], keys1[u], vals1[u] = spread(queries[part]), keys[part], vals[part]
        scores = [dot(queries2[u], keys1[u], 1, 1) * head_scale for u in here]
        for u, score in zip(here, scores):
            e = jnp.exp(score - jnp.max(score, -1, keepdims=True))
            probs[u] = e / jnp.sum(e, -1, keepdims=True)
            half[u] = probs[u].astype(bf16)
        context = [gather(dot(half[u], vals1[u])) * counts[u[0]] for u in here]
        left_ref[1, cols] = jnp.concatenate(context, 0).astype(bf16).T
        if j == 0 and not mutual:
            pl.semaphore_wait(barrier, 2 + steps)
        part = pl.ds(j * LANES, LANES)
        track(left_ref[1, part], cot, last, part, j)
        track_copy(0, j).start()

    loads["w3"].wait()
    context_grad = (dot(cot, weights_ref[3], 1, 1) * proj_scale).astype(bf16)
    weighted = [unit_rows[i * seq : (i + 1) * seq] * counts[i] for i in range(pool)]
    left_ref[0] = jnp.concatenate(weighted, 0).T.astype(bf16)
    queries2, keys1, vals1, probs, half = [
        [found[u] for u in units] for found in (queries2, keys1, vals1, probs, half)
    ]
    grads2 = [spread(context_grad[at]) for at in spots]
    for n, at in enumerate(spots):
        right_ref[2, at[0], at[1]] = dot(half[n], grads2[n], 0, 0).astype(bf16)
    loads["r2"].wait()
    each_block(1, 2, track_value)
    probs_grad = [dot(g, v, 1, 1) for g, v in zip(grads2, vals1)]
    score_grad = []
    for p, g in zip(probs, probs_grad):
        inner = jnp.sum(g * p, -1, keepdims=True)
        score_grad.append((p * (g - inner) * head_scale).astype(bf16))
    for n, at in enumerate(spots):
        right_ref[0, at[0], at[1]] = gather(dot(score_grad[n], keys1[n])).astype(bf16)
        right_ref[1, at[0], at[1]] = dot(score_grad[n], queries2[n], 0, 0).astype(bf16)
    loads["r01"].wait()
    each_block(2, matrices, track_rest)

    def sum_copy(k):
        return pltpu.make_async_remote_copy(
            totals.at[k], totals_in.at[k], sum_send.at[0], sum_recv.at[k], (partners[k],), MESH
        )

    def sum_finish(k):
        sum_copy(k).wait()
        totals[k + 1] = totals[k] + totals_in[k]

    own_total = jnp.sum(jnp.sum(squares[...], 0, keepdims=True), 1, keepdims=True)
    totals[0] = jnp.broadcast_to(own_total, totals.shape[1:])
    entries = nodes * matrices * width * width

    def set_rms():
        rms_ref[0] = jnp.sqrt(totals[steps] / entries)

    def mix(m, part, c):
        @pl.when(c % per_matrix == 0)
        def _():
            track_copy(0, c, per_matrix).wait_recv()

        tracker = 0.5 * (tracked[c].astype(f32) + tracked_in[c].astype(f32))
        own = weights_ref[m, part].astype(f32)
        new_residue_ref[0, m, part] = (tracker - gradient[c]).astype(bf16)
        base = 0.5 * own - 0.5 * step_rate * tracker
        if mutual:
            await_sent(c)
            peer_sent = (sent_in[c].astype(f32) - step_rate * tracker).astype(bf16)
            new_weights_ref[0, m, part] = (base + 0.5 * peer_sent.astype(f32)).astype(bf16)
        else:
            sent[c] = (own - step_rate * tracker).astype(bf16)
            sent_copy(c).start()
            gradient[c] = base

    def finish(m, part, c):
        await_sent(c)
        new_weights_ref[0, m, part] = (gradient[c] + 0.5 * sent_in[c].astype(f32)).astype(bf16)

    def await_gone(c):
        track_copy(slot(c), c).wait_send()

    if mutual:
        for k in range(steps - 2):
            sum_copy(k).start()
            sum_finish(k)
        for n, k in enumerate([steps - 2, steps - 1]):
            sum_copy(k).start()
            each_block(2 + n, 3 + n, send_weights)
            each_block(n, n + 1, mix)
            sum_finish(k)
        set_rms()
        each_block(2, matrices, mix)
        track_copy(0, 0, chunks).wait_send()
    else:
        second = 0 if offset == 1 else me % 2
        ahead = second * (LAG - 1)
        held = 2 * per_matrix
        starts = [held + k * (chunks - held) // steps for k in range(steps)]
        for gone in range(per_matrix, held - LAG):
            await_gone(gone)
        for c in range(held, chunks):
            await_gone(c - LAG if c <= tail else c - LAG + ahead)
            if c == tail:

                @pl.when(second == 1)
                def _():
                    for gone in range(c - LAG + 1, c):
                        await_gone(gone)

            for k in range(steps):
                if starts[k] == c:
                    if k:
                        sum_finish(k - 1)
                    sum_copy(k).start()
            track_copy(slot(c), c).start()
        sum_finish(steps - 1)
        set_rms()
        each_block(0, matrices, mix)
        each_block(0, matrices, finish)
        track_copy(0, 0, per_matrix).wait_send()

        @pl.when(second == 0)
        def _():
            for gone in range(chunks - LAG, chunks - 1):
                await_gone(gone)

        await_gone(chunks - 1)
    sent_copy(0, chunks).wait_send()


def one_round(nodes, level, sample_ids, token_pool, cotangent_pool, weights, residue):
    pool, seq, width = token_pool.shape[1:]
    matrices = weights.shape[1]
    rows = pool * seq
    per_matrix = width // CHUNK_ROWS
    chunks = matrices * per_matrix
    steps = nodes.bit_length() - 1
    chunked = (chunks, CHUNK_ROWS, width)
    dma = pltpu.SemaphoreType.DMA
    new_weights, new_residue, grad_rms = pl.pallas_call(
        partial(round_kernel, nodes, 2**level),
        out_shape=(
            jax.ShapeDtypeStruct(weights.shape, bf16),
            jax.ShapeDtypeStruct(weights.shape, bf16),
            jax.ShapeDtypeStruct((1, 8, LANES), f32),
        ),
        in_specs=[HBM] * 5,
        out_specs=(VMEM, VMEM, VMEM),
        scratch_shapes=[
            pltpu.VMEM(sample_ids.shape, jnp.int32),
            pltpu.VMEM((pool, seq, width), bf16),
            pltpu.VMEM((pool, seq, width), bf16),
            pltpu.VMEM(weights.shape[1:], bf16),
            pltpu.VMEM(weights.shape[1:], bf16),
            pltpu.VMEM((2, width, rows), bf16),
            pltpu.VMEM((3, rows, width), bf16),
            pltpu.VMEM((rows, width), f32),
            pltpu.VMEM(chunked, f32),
            pltpu.VMEM(chunked, bf16),
            pltpu.VMEM(chunked, bf16),
            pltpu.VMEM(chunked, bf16),
            pltpu.VMEM(chunked, bf16),
            pltpu.VMEM((8, width), f32),
            pltpu.VMEM((steps + 1, 8, LANES), f32),
            pltpu.VMEM((steps, 8, LANES), f32),
            dma((10,)),
            dma((1 + per_matrix,)),
            dma((matrices,)),
            dma((1,)),
            dma((matrices - 1 + per_matrix,)),
            dma((1,)),
            dma((steps,)),
        ],
        compiler_params=pltpu.CompilerParams(
            collective_id=level, has_side_effects=True, vmem_limit_bytes=30 * 2**20
        ),
    )(sample_ids, token_pool, cotangent_pool, weights, residue)
    return new_weights, new_residue, grad_rms[0]


def write_kernel(weights_ref, residue_ref, rms_ref, weights_out, residue_out, rms_out, rms, rms_sem, sems):
    copies = []
    for n, (src, dst) in enumerate([(weights_ref, weights_out), (residue_ref, residue_out)]):
        for m in range(src.shape[1]):
            copies.append(pltpu.make_async_copy(src.at[0, m], dst.at[0, m], sems.at[n, m]))
    for copy in copies:
        copy.start()
    rms[0] = rms_ref[0, 0]
    copies.append(pltpu.make_async_copy(rms, rms_out, rms_sem))
    copies[-1].start()
    for copy in copies:
        copy.wait()


def write_out(new_weights, new_residue, grad_rms):
    shape = jax.ShapeDtypeStruct(new_weights.shape, bf16)
    dma = pltpu.SemaphoreType.DMA
    return pl.pallas_call(
        write_kernel,
        out_shape=(shape, shape, jax.ShapeDtypeStruct((1,), f32)),
        in_specs=[VMEM, VMEM, VMEM],
        out_specs=(HBM, HBM, HBM),
        scratch_shapes=[pltpu.SMEM((1,), f32), dma, dma((2, new_weights.shape[1]))],
        compiler_params=pltpu.CompilerParams(vmem_limit_bytes=8 * 2**20),
    )(new_weights, new_residue, grad_rms)


def per_device(round_index, sample_ids, token_pool, cotangent_pool, weights, residue):
    nodes = lax.axis_size("node")
    levels = nodes.bit_length() - 1
    new_weights, new_residue, grad_rms = lax.switch(
        round_index[0] % levels,
        [partial(one_round, nodes, level) for level in range(levels)],
        sample_ids,
        token_pool,
        cotangent_pool,
        weights,
        residue,
    )
    new_weights, new_residue, grad_rms = write_out(new_weights, new_residue, grad_rms)
    return (new_weights, new_residue, grad_rms[0])


def solution(mesh):
    placed = (
        P(),
        P("node", None),
        P("node", None, None, None),
        P("node", None, None, None),
        P("node", None, None, None),
        P("node", None, None, None),
    )
    return jax.shard_map(
        per_device,
        mesh=mesh,
        in_specs=placed,
        out_specs=(P("node", None, None, None), P("node", None, None, None), P()),
        check_vma=False,
    )
```

```python
from functools import partial

import jax
import jax.numpy as jnp
from jax import lax
from jax.experimental import pallas as pl
from jax.experimental.pallas import tpu as pltpu
from jax.sharding import PartitionSpec as P

HEAD_DIM = 64
LANES = 128
CHUNK_ROWS = 128
LAG = 3

epsilon = 1e-06
step_rate = 0.1

f32, bf16 = jnp.float32, jnp.bfloat16
MESH = pl.DeviceIdType.MESH
VMEM = pl.BlockSpec(memory_space=pltpu.VMEM)
HBM = pl.BlockSpec(memory_space=pltpu.HBM)


def dot(left, right, left_dim=1, right_dim=0):
    return lax.dot_general(
        left, right, (((left_dim,), (right_dim,)), ((), ())), preferred_element_type=f32
    )


def round_kernel(
    nodes,
    offset,
    ids_hbm,
    tokens_hbm,
    cot_hbm,
    weights_hbm,
    residue_hbm,
    new_weights_ref,
    new_residue_ref,
    rms_ref,
    ids_ref,
    tokens_ref,
    cot_ref,
    weights_ref,
    residue_ref,
    left_ref,
    right_ref,
    context_ref,
    gradient,
    tracked,
    tracked_in,
    sent,
    sent_in,
    squares,
    totals,
    totals_in,
    load_sems,
    track_send,
    track_recv,
    sent_send,
    sent_recv,
    sum_send,
    sum_recv,
):
    me = lax.axis_index("node")
    target = lax.rem(me + offset, nodes)
    source = lax.rem(me + nodes - offset, nodes)
    steps = nodes.bit_length() - 1
    mutual = 2 * offset == nodes
    strides = [2**k for k in range(steps)]
    if not mutual:
        strides = [offset] + [stride for stride in strides if stride != offset]
    partners = [me + stride * (1 - 2 * ((me // stride) % 2)) for stride in strides]

    pool, seq, width = tokens_ref.shape
    matrices = weights_ref.shape[0]
    rows = pool * seq
    pairs = width // LANES
    per_matrix = width // CHUNK_ROWS
    chunks = matrices * per_matrix
    proj_scale = width**-0.5
    head_scale = HEAD_DIM**-0.5
    last = matrices - 1
    tail = last * per_matrix

    head, rest = pl.ds(0, CHUNK_ROWS), pl.ds(CHUNK_ROWS, width - CHUNK_ROWS)
    head_cols, rest_cols = pl.ds(0, LANES), pl.ds(LANES, width - LANES)
    qkv = pl.ds(0, 3)
    moves = {
        "tokens": (tokens_hbm.at[0], tokens_ref),
        "w": (weights_hbm.at[0, qkv, :, head_cols], weights_ref.at[qkv, :, head_cols]),
        "ids": (ids_hbm, ids_ref),
        "cot": (cot_hbm.at[0], cot_ref),
        "r": (residue_hbm.at[0, 3, head], residue_ref.at[3, head]),
        "w+": (weights_hbm.at[0, qkv, :, rest_cols], weights_ref.at[qkv, :, rest_cols]),
        "r+": (residue_hbm.at[0, 3, rest], residue_ref.at[3, rest]),
        "w3": (weights_hbm.at[0, 3], weights_ref.at[3]),
        "r012": (residue_hbm.at[0, qkv], residue_ref.at[qkv]),
    }
    loads = {}
    for n, (name, move) in enumerate(moves.items()):
        loads[name] = pltpu.make_async_copy(*move, load_sems.at[n])
        loads[name].start()

    barrier = pltpu.get_barrier_semaphore()
    for other in [target, source] + partners:
        pl.semaphore_signal(barrier, inc=1, device_id=(other,), device_id_type=MESH)

    def track_copy(n, c, size=1):
        at = pl.ds(c, size)
        return pltpu.make_async_remote_copy(
            tracked.at[at],
            tracked_in.at[at],
            track_send.at[n],
            track_recv.at[c // per_matrix],
            (target,),
            MESH,
        )

    def slot(c):
        return 0 if mutual else 1 + c % per_matrix

    def sent_sem(c):
        return c // per_matrix + (c % per_matrix) * (c // tail)

    def sent_copy(c, size=1):
        at = pl.ds(c, size)
        return pltpu.make_async_remote_copy(
            sent.at[at], sent_in.at[at], sent_send.at[0], sent_recv.at[sent_sem(c)], (target,), MESH
        )

    def send_weights(m, part, c):
        pltpu.make_async_remote_copy(
            weights_hbm.at[0, m, part],
            sent_in.at[c],
            sent_send.at[0],
            sent_recv.at[sent_sem(c)],
            (target,),
            MESH,
        ).start()

    def await_sent(c):
        @pl.when(c >= tail)
        def _():
            sent_copy(c).wait_recv()

        @pl.when((c < tail) & (c % per_matrix == 0))
        def _():
            sent_copy(c, per_matrix).wait_recv()

    def each_block(first, end, body):
        @pl.loop(first * per_matrix, end * per_matrix)
        def _(c):
            body(last - c // per_matrix, pl.ds((c % per_matrix) * CHUNK_ROWS, CHUNK_ROWS), c)

    if mutual:
        pl.semaphore_wait(barrier, 2 + steps)
        each_block(0, 2, send_weights)

    loads["tokens"].wait()
    values = tokens_ref[...].reshape(rows, width).astype(f32)
    centered = values - jnp.mean(values, -1, keepdims=True)
    variance = jnp.mean(centered * centered, -1, keepdims=True)
    unit_rows = centered * lax.rsqrt(variance + epsilon)
    normed = unit_rows.astype(bf16)
    first = lax.broadcasted_iota(jnp.int32, (seq, LANES), 1) < HEAD_DIM
    units = [(i, j) for i in range(pool) for j in range(pairs)]
    spots = [
        (slice(i * seq, (i + 1) * seq), slice(j * LANES, (j + 1) * LANES)) for i, j in units
    ]

    def spread(block):
        zero = jnp.zeros_like(block)
        return jnp.concatenate([jnp.where(first, block, zero), jnp.where(first, zero, block)], 0)

    def gather(block):
        return jnp.where(first, block[:seq], block[seq:])

    def track(left, right, m, part, c):
        grad = dot(left, right) * proj_scale
        gradient[c] = grad
        tracked[c] = (residue_ref[m, part].astype(f32) + grad).astype(bf16)
        squares[...] += jnp.sum((grad * grad).reshape(-1, 8, width), 0)

    def track_value(m, part, c):
        track(left_ref[0, part], right_ref[2], m, part, c)
        track_copy(slot(c), c).start()

    def track_rest(m, part, c):
        track(left_ref[0, part], right_ref[m], m, part, c)
        if mutual:
            track_copy(slot(c), c).start()

    loads["ids"].wait()
    ids = ids_ref[...]
    counts = [jnp.sum((ids == image).astype(f32), 1, keepdims=True) for image in range(pool)]
    loads["cot"].wait()
    cot = cot_ref[...].reshape(rows, width)
    squares[...] = jnp.zeros_like(squares)
    queries2, keys1, vals1, probs, half = {}, {}, {}, {}, {}
    for j in range(pairs):
        cols = slice(j * LANES, (j + 1) * LANES)
        if j < 2:
            loads["w+" if j else "w"].wait()
            loads["r+" if j else "r"].wait()
        queries, keys, vals = [
            (dot(normed, weights_ref[m, :, cols]) * proj_scale).astype(bf16) for m in range(3)
        ]
        here = [(i, j) for i in range(pool)]
        for i, u in enumerate(here):
            part = slice(i * seq, (i + 1) * seq)
            queries2[u], keys1[u], vals1[u] = spread(queries[part]), keys[part], vals[part]
        scores = [dot(queries2[u], keys1[u], 1, 1) * head_scale for u in here]
        for u, score in zip(here, scores):
            e = jnp.exp(score - jnp.max(score, -1, keepdims=True))
            probs[u] = e / jnp.sum(e, -1, keepdims=True)
            half[u] = probs[u].astype(bf16)
        context = [gather(dot(half[u], vals1[u])) * counts[u[0]] for u in here]
        left_ref[1, cols] = jnp.concatenate(context, 0).astype(bf16).T
        if j == 0 and not mutual:
            pl.semaphore_wait(barrier, 2 + steps)
        part = pl.ds(j * LANES, LANES)
        track(left_ref[1, part], cot, last, part, j)
        track_copy(0, j).start()

    loads["w3"].wait()
    context_grad = (dot(cot, weights_ref[3], 1, 1) * proj_scale).astype(bf16)
    weighted = [unit_rows[i * seq : (i + 1) * seq] * counts[i] for i in range(pool)]
    left_ref[0] = jnp.concatenate(weighted, 0).T.astype(bf16)
    queries2, keys1, vals1, probs, half = [
        [found[u] for u in units] for found in (queries2, keys1, vals1, probs, half)
    ]
    grads2 = [spread(context_grad[at]) for at in spots]
    for n, at in enumerate(spots):
        right_ref[2, at[0], at[1]] = dot(half[n], grads2[n], 0, 0).astype(bf16)
    loads["r012"].wait()
    each_block(1, 2, track_value)
    probs_grad = [dot(g, v, 1, 1) for g, v in zip(grads2, vals1)]
    score_grad = []
    for p, g in zip(probs, probs_grad):
        inner = jnp.sum(g * p, -1, keepdims=True)
        score_grad.append((p * (g - inner) * head_scale).astype(bf16))
    for n, at in enumerate(spots):
        right_ref[0, at[0], at[1]] = gather(dot(score_grad[n], keys1[n])).astype(bf16)
        right_ref[1, at[0], at[1]] = dot(score_grad[n], queries2[n], 0, 0).astype(bf16)
    each_block(2, matrices, track_rest)

    def sum_copy(k):
        return pltpu.make_async_remote_copy(
            totals.at[k], totals_in.at[k], sum_send.at[0], sum_recv.at[k], (partners[k],), MESH
        )

    def sum_finish(k):
        sum_copy(k).wait()
        totals[k + 1] = totals[k] + totals_in[k]

    own_total = jnp.sum(jnp.sum(squares[...], 0, keepdims=True), 1, keepdims=True)
    totals[0] = jnp.broadcast_to(own_total, totals.shape[1:])
    entries = nodes * matrices * width * width

    def set_rms():
        rms_ref[0] = jnp.broadcast_to(jnp.sqrt(totals[steps] / entries), rms_ref.shape[1:])

    def mix(m, part, c):
        @pl.when(c % per_matrix == 0)
        def _():
            track_copy(0, c, per_matrix).wait_recv()

        tracker = 0.5 * (tracked[c].astype(f32) + tracked_in[c].astype(f32))
        own = weights_ref[m, part].astype(f32)
        new_residue_ref[0, m, part] = (tracker - gradient[c]).astype(bf16)
        base = 0.5 * own - 0.5 * step_rate * tracker
        if mutual:
            await_sent(c)
            peer_sent = (sent_in[c].astype(f32) - step_rate * tracker).astype(bf16)
            new_weights_ref[0, m, part] = (base + 0.5 * peer_sent.astype(f32)).astype(bf16)
        else:
            sent[c] = (own - step_rate * tracker).astype(bf16)
            sent_copy(c).start()
            gradient[c] = base

    def finish(m, part, c):
        await_sent(c)
        new_weights_ref[0, m, part] = (gradient[c] + 0.5 * sent_in[c].astype(f32)).astype(bf16)

    def await_gone(c):
        track_copy(slot(c), c).wait_send()

    if mutual:
        for k in range(steps - 2):
            sum_copy(k).start()
            sum_finish(k)
        for n, k in enumerate([steps - 2, steps - 1]):
            sum_copy(k).start()
            each_block(2 + n, 3 + n, send_weights)
            each_block(n, n + 1, mix)
            sum_finish(k)
        set_rms()
        each_block(2, matrices, mix)
        track_copy(0, 0, chunks).wait_send()
    else:
        second = 0 if offset == 1 else me % 2
        ahead = second * (LAG - 1)
        held = 2 * per_matrix
        starts = [held + k * (chunks - held) // steps for k in range(steps)]
        for gone in range(per_matrix, held - LAG):
            await_gone(gone)
        for c in range(held, chunks):
            await_gone(c - LAG if c <= tail else c - LAG + ahead)
            if c == tail:

                @pl.when(second == 1)
                def _():
                    for gone in range(c - LAG + 1, c):
                        await_gone(gone)

            for k in range(steps):
                if starts[k] == c:
                    if k:
                        sum_finish(k - 1)
                    sum_copy(k).start()
            track_copy(slot(c), c).start()
        sum_finish(steps - 1)
        set_rms()
        each_block(0, matrices, mix)
        each_block(0, matrices, finish)
        track_copy(0, 0, per_matrix).wait_send()

        @pl.when(second == 0)
        def _():
            for gone in range(chunks - LAG, chunks - 1):
                await_gone(gone)

        await_gone(chunks - 1)
    sent_copy(0, chunks).wait_send()


def one_round(nodes, level, sample_ids, token_pool, cotangent_pool, weights, residue):
    pool, seq, width = token_pool.shape[1:]
    matrices = weights.shape[1]
    rows = pool * seq
    per_matrix = width // CHUNK_ROWS
    chunks = matrices * per_matrix
    steps = nodes.bit_length() - 1
    chunked = (chunks, CHUNK_ROWS, width)
    dma = pltpu.SemaphoreType.DMA
    new_weights, new_residue, grad_rms = pl.pallas_call(
        partial(round_kernel, nodes, 2**level),
        out_shape=(
            jax.ShapeDtypeStruct(weights.shape, bf16),
            jax.ShapeDtypeStruct(weights.shape, bf16),
            jax.ShapeDtypeStruct((1, 8, LANES), f32),
        ),
        in_specs=[HBM] * 5,
        out_specs=(VMEM, VMEM, VMEM),
        scratch_shapes=[
            pltpu.VMEM(sample_ids.shape, jnp.int32),
            pltpu.VMEM((pool, seq, width), bf16),
            pltpu.VMEM((pool, seq, width), bf16),
            pltpu.VMEM(weights.shape[1:], bf16),
            pltpu.VMEM(weights.shape[1:], bf16),
            pltpu.VMEM((2, width, rows), bf16),
            pltpu.VMEM((3, rows, width), bf16),
            pltpu.VMEM((rows, width), f32),
            pltpu.VMEM(chunked, f32),
            pltpu.VMEM(chunked, bf16),
            pltpu.VMEM(chunked, bf16),
            pltpu.VMEM(chunked, bf16),
            pltpu.VMEM(chunked, bf16),
            pltpu.VMEM((8, width), f32),
            pltpu.VMEM((steps + 1, 1, LANES), f32),
            pltpu.VMEM((steps, 1, LANES), f32),
            dma((9,)),
            dma((1 + per_matrix,)),
            dma((matrices,)),
            dma((1,)),
            dma((matrices - 1 + per_matrix,)),
            dma((1,)),
            dma((steps,)),
        ],
        compiler_params=pltpu.CompilerParams(
            collective_id=level, has_side_effects=True, vmem_limit_bytes=30 * 2**20
        ),
    )(sample_ids, token_pool, cotangent_pool, weights, residue)
    return new_weights, new_residue, grad_rms[0]


def write_kernel(weights_ref, residue_ref, rms_ref, weights_out, residue_out, rms_out, rms, rms_sem, sems):
    copies = []
    for n, (src, dst) in enumerate([(weights_ref, weights_out), (residue_ref, residue_out)]):
        for m in range(src.shape[1]):
            copies.append(pltpu.make_async_copy(src.at[0, m], dst.at[0, m], sems.at[n, m]))
    for copy in copies:
        copy.start()
    rms[0] = rms_ref[0, 0]
    copies.append(pltpu.make_async_copy(rms, rms_out, rms_sem))
    copies[-1].start()
    for copy in copies:
        copy.wait()


def write_out(new_weights, new_residue, grad_rms):
    shape = jax.ShapeDtypeStruct(new_weights.shape, bf16)
    dma = pltpu.SemaphoreType.DMA
    return pl.pallas_call(
        write_kernel,
        out_shape=(shape, shape, jax.ShapeDtypeStruct((1,), f32)),
        in_specs=[VMEM, VMEM, VMEM],
        out_specs=(HBM, HBM, HBM),
        scratch_shapes=[pltpu.SMEM((1,), f32), dma, dma((2, new_weights.shape[1]))],
        compiler_params=pltpu.CompilerParams(vmem_limit_bytes=8 * 2**20),
    )(new_weights, new_residue, grad_rms)


def per_device(round_index, sample_ids, token_pool, cotangent_pool, weights, residue):
    nodes = lax.axis_size("node")
    levels = nodes.bit_length() - 1
    new_weights, new_residue, grad_rms = lax.switch(
        round_index[0] % levels,
        [partial(one_round, nodes, level) for level in range(levels)],
        sample_ids,
        token_pool,
        cotangent_pool,
        weights,
        residue,
    )
    new_weights, new_residue, grad_rms = write_out(new_weights, new_residue, grad_rms)
    return (new_weights, new_residue, grad_rms[0])


def solution(mesh):
    placed = (
        P(),
        P("node", None),
        P("node", None, None, None),
        P("node", None, None, None),
        P("node", None, None, None),
        P("node", None, None, None),
    )
    return jax.shard_map(
        per_device,
        mesh=mesh,
        in_specs=placed,
        out_specs=(P("node", None, None, None), P("node", None, None, None), P()),
        check_vma=False,
    )
```
